32 devices in a mesh: dom: 32 (over z, y, x, core).
Axes of the slice: x: 2, y: 2, z: 4, core: 2. Of those that a mesh axis runs over, the one named last changes fastest.
Arguments:
- tracers: float32 [20, 8, 32768], P(None, None, 'dom'), may hold values from -6 to 6
- mass_flux: float32 [3, 8, 32768], P(None, None, 'dom'), may hold values from -6 to 6
- lsq_coeff: float32 [2, 3, 32768], P(None, None, 'dom'), may hold values from -3 to 3
- own_offset: float32 [2, 3, 8, 32768], P(None, None, None, 'dom'), may hold values from -1.5 to 1.5
- far_offset: float32 [2, 3, 8, 32768], P(None, None, None, 'dom'), may hold values from -1.5 to 1.5
- inv_mass: float32 [8, 32768], P(None, 'dom'), may hold values from 0.25 to 1
- neighbour: int32 [3, 32768], P(None, 'dom'), may hold values from 0 to 1791, as said below
- send_cells: int32 [6, 4096], P(None, 'dom'), may hold values from 0 to 1023, as said below
Outputs:
- updated: float32 [20, 8, 32768], P(None, None, 'dom')
The draws below stay inside these ranges and needn't reach their ends.
Inputs may be any that keep to these rules, and one draw needn't show every extreme that they name: For each domain, entries index its 1024 own cells followed by 6 received blocks of 128 slots; every referenced received slot holds a real cell of the sending domain, the unused tail of a block is never referenced, and for every neighbour slot some domain references a block in full. `send_cells`: each block of 128 entries (one sending domain, one neighbour slot) lists distinct own cells of the sending domain, as local indices.
All inputs are finite; a program needn't handle non-finite values.
Results may differ from the reference program's by a relative error of at most 0.0003.
Values sent between devices are 32-bit elements; how exact they have to be, the bound alone decides.
No kernel may reach another device: no remote copies, remote signals or barrier semaphores. Data moves between devices by JAX's collectives and lax.ppermute only.
A program may use at most 64 MiB of HBM per device.

```python
import math
import jax
import jax.numpy as jnp

TRC = 20
LEV = 8
CEL_DEV = 1024
PEERS = 6
HALO = 128
NCELL = 32768


def peer_shift_drawn(peer_slot):
    return (peer_slot // 2 + 1) * (1 - 2 * (peer_slot % 2))


def mesh_tables(key):
    devices = NCELL // CEL_DEV
    offsets = jnp.array([peer_shift_drawn(peer_slot) for peer_slot in range(PEERS)], jnp.int32)
    fewest = max(1, HALO // 4)
    counts = jax.random.randint(jax.random.fold_in(key, 101), (devices, PEERS), fewest, HALO + 1)
    full_rank = jax.random.randint(jax.random.fold_in(key, 102), (PEERS,), 0, devices)
    counts = jnp.where(jnp.arange(devices)[:, None] == full_rank[None, :], HALO, counts)
    send_keys = jax.random.split(jax.random.fold_in(key, 103), devices * PEERS)

    def pick_cells(subkey):
        return jax.random.permutation(subkey, CEL_DEV)[:HALO]
    chosen = jax.vmap(pick_cells)(send_keys)
    send_table = chosen.reshape(devices, PEERS, HALO).transpose(1, 0, 2).reshape(PEERS, devices * HALO)
    sender = (jnp.arange(devices)[:, None] - offsets[None, :]) % devices
    recv_counts = counts[sender, jnp.arange(PEERS)[None, :]]
    slot_range = jnp.arange(HALO)
    usable = slot_range[None, None, :] < recv_counts[:, :, None]
    values = CEL_DEV + jnp.arange(PEERS)[:, None] * HALO + slot_range[None, :]
    slot_table = jnp.where(usable, values[None], -1).reshape(devices, PEERS * HALO)
    filler = jnp.full((devices, 3 * CEL_DEV - PEERS * HALO), -1, slot_table.dtype)
    padded = jnp.concatenate([slot_table, filler], axis=1)
    place_keys = jax.random.split(jax.random.fold_in(key, 104), devices)

    def place_row(subkey, slot_row):
        return slot_row[jax.random.permutation(subkey, 3 * CEL_DEV)]
    placed = jax.vmap(place_row)(place_keys, padded).reshape(devices, 3, CEL_DEV)
    jumps = jax.random.randint(jax.random.fold_in(key, 105), (devices, 3, CEL_DEV), 1, CEL_DEV)
    local_pick = (jnp.arange(CEL_DEV)[None, None, :] + jumps) % CEL_DEV
    neighbour_table = jnp.where(placed >= 0, placed, local_pick).transpose(1, 0, 2).reshape(3, devices * CEL_DEV)
    return (neighbour_table.astype(jnp.int32), send_table.astype(jnp.int32))


def draw_neighbour(key, part):
    return mesh_tables(key)[0]


def draw_send_cells(key, part):
    return mesh_tables(key)[1]


def steps_of(own_key, extent, cuts, low, high):
    def one(position, blocks):
        draws = jax.random.uniform(jax.random.fold_in(jax.random.fold_in(own_key, 6), position), (blocks,), jnp.float32, low / len(cuts), high / len(cuts))
        return jnp.repeat(jnp.exp(draws), extent[position] // blocks).reshape((-1,) + (1,) * (len(extent) - position - 1))

    level = one(*cuts[0])
    for cut in cuts[1:]:
        level = level * one(*cut)
    return level


def noise(rng, dims, width, reach, cuts=(), held_as=jnp.bfloat16):
    result = width * jax.random.normal(rng, dims, jnp.float32)
    if cuts:
        result = result * steps_of(rng, dims, cuts, -0.22, 0.18)
    return jnp.clip(result, -reach, reach).astype(held_as)


def setup_inputs(seed: int = 0) -> dict:
    arg_keys = jax.random.split(jax.random.key(seed), 9)
    tracers = noise(arg_keys[0], (TRC, LEV, NCELL), 1.0, 6.0, ((2, 32),), jnp.float32)
    mass_flux = noise(arg_keys[1], (3, LEV, NCELL), 1.0, 6.0, ((2, 32),), jnp.float32)
    lsq_coeff = noise(arg_keys[2], (2, 3, NCELL), 0.5, 3.0, ((2, 32),), jnp.float32)
    own_offset = noise(arg_keys[3], (2, 3, LEV, NCELL), 0.3, 1.5, ((3, 32),), jnp.float32)
    far_offset = noise(arg_keys[4], (2, 3, LEV, NCELL), 0.3, 1.5, ((3, 32),), jnp.float32)
    inv_mass = jnp.clip(jnp.exp(math.log(1.0) - 1.3862944 * jax.random.uniform(arg_keys[5], (LEV, NCELL), jnp.float32) ** steps_of(arg_keys[5], (LEV, NCELL), ((1, 32),), -0.2, 0.2)), 0.25, 1.0)
    neighbour = draw_neighbour(jax.random.fold_in(arg_keys[8], 71), 0)
    send_cells = draw_send_cells(jax.random.fold_in(arg_keys[8], 71), 0)
    return {"tracers": tracers, "mass_flux": mass_flux, "lsq_coeff": lsq_coeff, "own_offset": own_offset, "far_offset": far_offset, "inv_mass": inv_mass, "neighbour": neighbour, "send_cells": send_cells}


def peer_shift(peer_slot):
    return (peer_slot // 2 + 1) * (1 - 2 * (peer_slot % 2))


def reference(tracers, mass_flux, lsq_coeff, own_offset, far_offset, inv_mass, neighbour, send_cells):
    devices = NCELL // CEL_DEV
    offsets = jnp.array([peer_shift(peer_slot) for peer_slot in range(PEERS)], jnp.int32)
    owners = jnp.arange(devices, dtype=jnp.int32)
    sender = ((owners[:, None] - offsets[None, :]) % devices).astype(jnp.int32)
    blocks = send_cells.reshape(PEERS, devices, HALO).astype(jnp.int32)
    remote = blocks[jnp.arange(PEERS, dtype=jnp.int32)[None, :], sender, :]
    remote = (remote + sender[:, :, None] * CEL_DEV).astype(jnp.int32)
    own_ids = (owners[:, None] * CEL_DEV + jnp.arange(CEL_DEV, dtype=jnp.int32)[None, :]).astype(jnp.int32)
    lookup = jnp.concatenate([own_ids, remote.reshape(devices, PEERS * HALO)], axis=1).astype(jnp.int32)
    local_ids = neighbour.reshape(3, devices, CEL_DEV).astype(jnp.int32)
    wide_lookup = jnp.broadcast_to(lookup[None], (3, devices, lookup.shape[1]))
    global_ids = jnp.take_along_axis(wide_lookup, local_ids, axis=2).reshape(3, NCELL).astype(jnp.int32)
    beside = [jnp.take(tracers, global_ids[edge_slot], axis=2) for edge_slot in range(3)]
    gradient = None
    for edge_slot in range(3):
        summand = lsq_coeff[:, edge_slot][:, None, None, :] * (beside[edge_slot] - tracers)[None]
        gradient = summand if gradient is None else gradient + summand
    outflow = jnp.zeros_like(tracers)
    for edge_slot in range(3):
        far_value = beside[edge_slot]
        far_grad = jnp.take(gradient, global_ids[edge_slot], axis=3)
        own_face = tracers + gradient[0] * own_offset[0, edge_slot] + gradient[1] * own_offset[1, edge_slot]
        far_face = far_value + far_grad[0] * far_offset[0, edge_slot] + far_grad[1] * far_offset[1, edge_slot]
        side_flux = mass_flux[edge_slot]
        face_value = jnp.where(side_flux > 0, own_face, far_face)
        face_value = jnp.clip(face_value, jnp.minimum(tracers, far_value), jnp.maximum(tracers, far_value))
        outflow = outflow + side_flux * face_value
    return tracers - inv_mass * outflow
```

```python
import functools

import jax
import jax.numpy as jnp
from jax import lax
from jax.experimental import pallas as pl
from jax.sharding import PartitionSpec as P

F32 = jnp.float32
BF16 = jnp.bfloat16
STEP = 256


def passed_along(block, axis, distance):
    devices = range(lax.axis_size(axis))
    route = [((i - distance) % len(devices), i) for i in devices]
    return lax.ppermute(block, axis, route)


def peer_shift(peer_slot):
    return (peer_slot // 2 + 1) * (1 - 2 * (peer_slot % 2))


def exchange(blocks):
    return [passed_along(block, "dom", peer_shift(slot)) for slot, block in enumerate(blocks)]


def halves(x):
    high = x.astype(BF16)
    low = (x - high.astype(F32)).astype(BF16)
    return jnp.concatenate([high, low], axis=0)


def selector(index_row, first, count):
    place = lax.broadcasted_iota(jnp.int32, (count, index_row.shape[1]), 0) + first
    return jnp.where(place == index_row, 1.0, 0.0).astype(BF16)


def picked(parts, chooser):
    both = jnp.dot(parts, chooser, preferred_element_type=F32)
    rows = both.shape[0] // 2
    return both[:rows] + both[rows:]


def steps(cell_count):
    width = STEP if cell_count % STEP == 0 else cell_count
    return [(at, at + width) for at in range(0, cell_count, width)]


def pack_kernel(flat_ref, send_ref, *out_refs):
    parts = halves(flat_ref[...])
    cell_count = parts.shape[1]
    for slot, out_ref in enumerate(out_refs):
        out_ref[...] = picked(parts, selector(send_ref[slot : slot + 1, :], 0, cell_count))


def near_kernel(flat_ref, near_ref, out_ref):
    parts = halves(flat_ref[...])
    cell_count = parts.shape[1]
    for edge in range(3):
        for lo, hi in steps(cell_count):
            chooser = selector(near_ref[edge : edge + 1, lo:hi], 0, cell_count)
            out_ref[edge, :, lo:hi] = picked(parts, chooser)


def gradient_kernel(peer_count, flat_ref, own_ref, lsq_ref, near_ref, send_ref, *refs):
    got_refs = refs[:peer_count]
    beside_ref, grad_ref = refs[peer_count : peer_count + 2]
    out_refs = refs[peer_count + 2 :]
    rows, cell_count = flat_ref.shape
    got = jnp.concatenate([halves(ref[...]) for ref in got_refs], axis=1)
    halo_count = got.shape[1]
    for lo, hi in steps(cell_count):
        centre = flat_ref[:, lo:hi]
        sums = [None, None]
        for edge in range(3):
            chooser = selector(near_ref[edge : edge + 1, lo:hi], cell_count, halo_count)
            value = own_ref[edge, :, lo:hi] + picked(got, chooser)
            beside_ref[edge, :, lo:hi] = value
            change = value - centre
            for comp in range(2):
                term = lsq_ref[comp, edge : edge + 1, lo:hi] * change
                sums[comp] = term if sums[comp] is None else sums[comp] + term
        grad_ref[:rows, lo:hi] = sums[0]
        grad_ref[rows:, lo:hi] = sums[1]
    parts = halves(grad_ref[...])
    for slot, out_ref in enumerate(out_refs):
        out_ref[...] = picked(parts, selector(send_ref[slot : slot + 1, :], 0, cell_count))


def spread_levels(coeff, rows):
    return jnp.tile(coeff, (rows // coeff.shape[0], 1))


def own_kernel(flat_ref, grad_ref, beside_ref, near_ref, flux_ref, own_off_ref, far_off_ref, far_ref, sum_ref):
    rows, cell_count = flat_ref.shape
    parts = halves(grad_ref[...])
    for lo, hi in steps(cell_count):
        centre = flat_ref[:, lo:hi]
        first = grad_ref[:rows, lo:hi]
        second = grad_ref[rows:, lo:hi]
        total = None
        for edge in range(3):
            chooser = selector(near_ref[edge : edge + 1, lo:hi], 0, cell_count)
            far = picked(parts, chooser)
            value = beside_ref[edge, :, lo:hi]
            far_ref[edge, :, lo:hi] = (
                value
                + far[:rows] * spread_levels(far_off_ref[0, edge, :, lo:hi], rows)
                + far[rows:] * spread_levels(far_off_ref[1, edge, :, lo:hi], rows)
            )
            face = (
                centre
                + first * spread_levels(own_off_ref[0, edge, :, lo:hi], rows)
                + second * spread_levels(own_off_ref[1, edge, :, lo:hi], rows)
            )
            face = jnp.clip(face, jnp.minimum(centre, value), jnp.maximum(centre, value))
            outward = spread_levels(jnp.maximum(flux_ref[edge, :, lo:hi], 0.0), rows)
            total = outward * face if total is None else total + outward * face
        sum_ref[:, lo:hi] = total


def far_kernel(peer_count, flat_ref, beside_ref, far_ref, sum_ref, near_ref, flux_ref, far_off_ref, mass_ref, *refs):
    got_refs, out_ref = refs[:peer_count], refs[peer_count]
    rows, cell_count = flat_ref.shape
    got = jnp.concatenate([halves(ref[...]) for ref in got_refs], axis=1)
    halo_count = got.shape[1]
    for lo, hi in steps(cell_count):
        centre = flat_ref[:, lo:hi]
        total = sum_ref[:, lo:hi]
        for edge in range(3):
            chooser = selector(near_ref[edge : edge + 1, lo:hi], cell_count, halo_count)
            far = picked(got, chooser)
            value = beside_ref[edge, :, lo:hi]
            face = (
                far_ref[edge, :, lo:hi]
                + far[:rows] * spread_levels(far_off_ref[0, edge, :, lo:hi], rows)
                + far[rows:] * spread_levels(far_off_ref[1, edge, :, lo:hi], rows)
            )
            face = jnp.clip(face, jnp.minimum(centre, value), jnp.maximum(centre, value))
            inward = spread_levels(jnp.minimum(flux_ref[edge, :, lo:hi], 0.0), rows)
            total = total + inward * face
        out_ref[:, lo:hi] = centre - spread_levels(mass_ref[:, lo:hi], rows) * total


def run(kernel, outs, flops, *operands):
    moved = sum(4 * x.size for x in operands) + sum(4 * x.size for x in outs)
    return pl.pallas_call(
        kernel,
        out_shape=outs,
        cost_estimate=pl.CostEstimate(flops=flops, bytes_accessed=moved, transcendentals=0),
    )(*operands)


def on_device(
    tracers, mass_flux, lsq_coeff, own_offset, far_offset, inv_mass, neighbour, send_cells
):
    tracer_count, level_count, cell_count = tracers.shape
    rows = tracer_count * level_count
    peer_count, halo_width = send_cells.shape
    halo_count = peer_count * halo_width
    flat = tracers.reshape(rows, cell_count)

    def like(*shape):
        return jax.ShapeDtypeStruct(shape, F32)

    def work(height, depth, width):
        return 4 * height * depth * width

    sent = run(
        pack_kernel,
        [like(rows, halo_width)] * peer_count,
        work(rows, cell_count, halo_count),
        flat,
        send_cells,
    )
    got = exchange(sent)
    own_beside = run(
        near_kernel,
        [like(3, rows, cell_count)],
        work(rows, cell_count, 3 * cell_count),
        flat,
        neighbour,
    )[0]
    beside, grad, *grad_sent = run(
        functools.partial(gradient_kernel, peer_count),
        [like(3, rows, cell_count), like(2 * rows, cell_count)]
        + [like(2 * rows, halo_width)] * peer_count,
        work(rows, halo_count, 5 * cell_count),
        flat,
        own_beside,
        lsq_coeff,
        neighbour,
        send_cells,
        *got,
    )
    grad_got = exchange(grad_sent)
    far_part, own_sum = run(
        own_kernel,
        [like(3, rows, cell_count), like(rows, cell_count)],
        work(2 * rows, cell_count, 3 * cell_count),
        flat,
        grad,
        beside,
        neighbour,
        mass_flux,
        own_offset,
        far_offset,
    )
    updated = run(
        functools.partial(far_kernel, peer_count),
        [like(rows, cell_count)],
        work(2 * rows, halo_count, 3 * cell_count),
        flat,
        beside,
        far_part,
        own_sum,
        neighbour,
        mass_flux,
        far_offset,
        inv_mass,
        *grad_got,
    )[0]
    return updated.reshape(tracers.shape)


def solution(mesh):
    placed = (
        P(None, None, "dom"),
        P(None, None, "dom"),
        P(None, None, "dom"),
        P(None, None, None, "dom"),
        P(None, None, None, "dom"),
        P(None, "dom"),
        P(None, "dom"),
        P(None, "dom"),
    )
    return jax.shard_map(
        on_device, mesh=mesh, in_specs=placed, out_specs=P(None, None, "dom"), check_vma=False
    )
```

```python
import functools

import jax
import jax.numpy as jnp
from jax import lax
from jax.experimental import pallas as pl
from jax.experimental.pallas import tpu as pltpu
from jax.sharding import PartitionSpec as P

F32 = jnp.float32
BF16 = jnp.bfloat16
STEP = 256
GRANT = 24 * 2**20


def passed_along(block, axis, distance):
    devices = range(lax.axis_size(axis))
    route = [((i - distance) % len(devices), i) for i in devices]
    return lax.ppermute(block, axis, route)


def peer_shift(peer_slot):
    return (peer_slot // 2 + 1) * (1 - 2 * (peer_slot % 2))


def one_way(slot_count):
    return sorted(range(slot_count), key=lambda slot: (slot % 2, slot))


def by_slot(refs):
    return [refs[one_way(len(refs)).index(slot)] for slot in range(len(refs))]


def exchange(blocks):
    order = one_way(len(blocks))
    return [passed_along(block, "dom", peer_shift(slot)) for slot, block in zip(order, blocks)]


def halves(x):
    high = x.astype(BF16)
    low = (x - high.astype(F32)).astype(BF16)
    return jnp.concatenate([high, low], axis=0)


def selector(index_row, first, count):
    place = lax.broadcasted_iota(jnp.int32, (count, index_row.shape[1]), 0) + first
    return jnp.where(place == index_row, 1.0, 0.0).astype(BF16)


def picked(parts, chooser):
    both = jnp.dot(parts, chooser, preferred_element_type=F32)
    rows = both.shape[0] // 2
    return both[:rows] + both[rows:]


def steps(cell_count):
    width = STEP if cell_count % STEP == 0 else cell_count
    return [(at, at + width) for at in range(0, cell_count, width)]


def pack_kernel(flat_ref, send_ref, *out_refs):
    parts = halves(flat_ref[...])
    cell_count = parts.shape[1]
    for slot, out_ref in enumerate(by_slot(out_refs)):
        out_ref[...] = picked(parts, selector(send_ref[slot : slot + 1, :], 0, cell_count))


def near_kernel(flat_ref, near_ref, out_ref):
    parts = halves(flat_ref[...])
    cell_count = parts.shape[1]
    for edge in range(3):
        for lo, hi in steps(cell_count):
            chooser = selector(near_ref[edge : edge + 1, lo:hi], 0, cell_count)
            out_ref[edge, :, lo:hi] = picked(parts, chooser)


def gradient_kernel(peer_count, flat_ref, own_ref, lsq_ref, near_ref, send_ref, *refs):
    got_refs = refs[:peer_count]
    beside_ref, grad_ref = refs[peer_count : peer_count + 2]
    out_refs = refs[peer_count + 2 :]
    rows, cell_count = flat_ref.shape
    got = jnp.concatenate([halves(ref[...]) for ref in by_slot(got_refs)], axis=1)
    halo_count = got.shape[1]
    for lo, hi in steps(cell_count):
        centre = flat_ref[:, lo:hi]
        sums = [None, None]
        for edge in range(3):
            chooser = selector(near_ref[edge : edge + 1, lo:hi], cell_count, halo_count)
            value = own_ref[edge, :, lo:hi] + picked(got, chooser)
            beside_ref[edge, :, lo:hi] = value
            change = value - centre
            for comp in range(2):
                term = lsq_ref[comp, edge : edge + 1, lo:hi] * change
                sums[comp] = term if sums[comp] is None else sums[comp] + term
        grad_ref[:rows, lo:hi] = sums[0]
        grad_ref[rows:, lo:hi] = sums[1]
    parts = halves(grad_ref[...])
    for slot, out_ref in enumerate(by_slot(out_refs)):
        out_ref[...] = picked(parts, selector(send_ref[slot : slot + 1, :], 0, cell_count))


def spread_levels(coeff, rows):
    return jnp.tile(coeff, (rows // coeff.shape[0], 1))


def own_kernel(flat_ref, grad_ref, beside_ref, near_ref, flux_ref, own_off_ref, far_off_ref, far_ref, sum_ref):
    rows, cell_count = flat_ref.shape
    parts = halves(grad_ref[...])
    for lo, hi in steps(cell_count):
        centre = flat_ref[:, lo:hi]
        first = grad_ref[:rows, lo:hi]
        second = grad_ref[rows:, lo:hi]
        total = None
        for edge in range(3):
            chooser = selector(near_ref[edge : edge + 1, lo:hi], 0, cell_count)
            far = picked(parts, chooser)
            value = beside_ref[edge, :, lo:hi]
            far_ref[edge, :, lo:hi] = (
                value
                + far[:rows] * spread_levels(far_off_ref[0, edge, :, lo:hi], rows)
                + far[rows:] * spread_levels(far_off_ref[1, edge, :, lo:hi], rows)
            )
            face = (
                centre
                + first * spread_levels(own_off_ref[0, edge, :, lo:hi], rows)
                + second * spread_levels(own_off_ref[1, edge, :, lo:hi], rows)
            )
            face = jnp.clip(face, jnp.minimum(centre, value), jnp.maximum(centre, value))
            outward = spread_levels(jnp.maximum(flux_ref[edge, :, lo:hi], 0.0), rows)
            total = outward * face if total is None else total + outward * face
        sum_ref[:, lo:hi] = total


def far_kernel(peer_count, flat_ref, beside_ref, far_ref, sum_ref, near_ref, flux_ref, far_off_ref, mass_ref, *refs):
    got_refs, out_ref = refs[:peer_count], refs[peer_count]
    rows, cell_count = flat_ref.shape
    got = jnp.concatenate([halves(ref[...]) for ref in by_slot(got_refs)], axis=1)
    halo_count = got.shape[1]
    for lo, hi in steps(cell_count):
        centre = flat_ref[:, lo:hi]
        total = sum_ref[:, lo:hi]
        for edge in range(3):
            chooser = selector(near_ref[edge : edge + 1, lo:hi], cell_count, halo_count)
            far = picked(got, chooser)
            value = beside_ref[edge, :, lo:hi]
            face = (
                far_ref[edge, :, lo:hi]
                + far[:rows] * spread_levels(far_off_ref[0, edge, :, lo:hi], rows)
                + far[rows:] * spread_levels(far_off_ref[1, edge, :, lo:hi], rows)
            )
            face = jnp.clip(face, jnp.minimum(centre, value), jnp.maximum(centre, value))
            inward = spread_levels(jnp.minimum(flux_ref[edge, :, lo:hi], 0.0), rows)
            total = total + inward * face
        out_ref[:, lo:hi] = centre - spread_levels(mass_ref[:, lo:hi], rows) * total


def run(kernel, outs, flops, *operands):
    moved = sum(4 * x.size for x in operands) + sum(4 * x.size for x in outs)
    return pl.pallas_call(
        kernel,
        out_shape=outs,
        compiler_params=pltpu.CompilerParams(vmem_limit_bytes=GRANT),
        cost_estimate=pl.CostEstimate(flops=flops, bytes_accessed=moved, transcendentals=0),
    )(*operands)


def on_device(
    tracers, mass_flux, lsq_coeff, own_offset, far_offset, inv_mass, neighbour, send_cells
):
    tracer_count, level_count, cell_count = tracers.shape
    rows = tracer_count * level_count
    peer_count, halo_width = send_cells.shape
    halo_count = peer_count * halo_width
    flat = tracers.reshape(rows, cell_count)

    def like(*shape):
        return jax.ShapeDtypeStruct(shape, F32)

    def work(height, depth, width):
        return 4 * height * depth * width

    sent = run(
        pack_kernel,
        [like(rows, halo_width)] * peer_count,
        work(rows, cell_count, halo_count),
        flat,
        send_cells,
    )
    got = exchange(sent)
    own_beside = run(
        near_kernel,
        [like(3, rows, cell_count)],
        work(rows, cell_count, 3 * cell_count),
        flat,
        neighbour,
    )[0]
    beside, grad, *grad_sent = run(
        functools.partial(gradient_kernel, peer_count),
        [like(3, rows, cell_count), like(2 * rows, cell_count)]
        + [like(2 * rows, halo_width)] * peer_count,
        work(rows, halo_count, 5 * cell_count),
        flat,
        own_beside,
        lsq_coeff,
        neighbour,
        send_cells,
        *got,
    )
    grad_got = exchange(grad_sent)
    far_part, own_sum = run(
        own_kernel,
        [like(3, rows, cell_count), like(rows, cell_count)],
        work(2 * rows, cell_count, 3 * cell_count),
        flat,
        grad,
        beside,
        neighbour,
        mass_flux,
        own_offset,
        far_offset,
    )
    updated = run(
        functools.partial(far_kernel, peer_count),
        [like(rows, cell_count)],
        work(2 * rows, halo_count, 3 * cell_count),
        flat,
        beside,
        far_part,
        own_sum,
        neighbour,
        mass_flux,
        far_offset,
        inv_mass,
        *grad_got,
    )[0]
    return updated.reshape(tracers.shape)


def solution(mesh):
    placed = (
        P(None, None, "dom"),
        P(None, None, "dom"),
        P(None, None, "dom"),
        P(None, None, None, "dom"),
        P(None, None, None, "dom"),
        P(None, "dom"),
        P(None, "dom"),
        P(None, "dom"),
    )
    return jax.shard_map(
        on_device, mesh=mesh, in_specs=placed, out_specs=P(None, None, "dom"), check_vma=False
    )
```

```python
import functools

import jax
import jax.numpy as jnp
from jax import lax
from jax.experimental import pallas as pl
from jax.experimental.pallas import tpu as pltpu
from jax.sharding import PartitionSpec as P

F32 = jnp.float32
BF16 = jnp.bfloat16
STEP = 256
GRANT = 24 * 2**20


def passed_along(block, axis, distance):
    devices = range(lax.axis_size(axis))
    route = [((i - distance) % len(devices), i) for i in devices]
    return lax.ppermute(block, axis, route)


def peer_shift(peer_slot):
    return (peer_slot // 2 + 1) * (1 - 2 * (peer_slot % 2))


def one_way(slot_count):
    return sorted(range(slot_count), key=lambda slot: (slot % 2, slot))


def by_slot(refs):
    return [refs[one_way(len(refs)).index(slot)] for slot in range(len(refs))]


def exchange(blocks):
    order = one_way(len(blocks))
    return [passed_along(block, "dom", peer_shift(slot)) for slot, block in zip(order, blocks)]


def halves(x):
    high = x.astype(BF16)
    low = (x - high.astype(F32)).astype(BF16)
    return jnp.concatenate([high, low], axis=0)


def selector(index_row, first, count):
    place = lax.broadcasted_iota(jnp.int32, (count, index_row.shape[1]), 0) + first
    return jnp.where(place == index_row, 1.0, 0.0).astype(BF16)


def picked(parts, chooser):
    both = jnp.dot(parts, chooser, preferred_element_type=F32)
    rows = both.shape[0] // 2
    return both[:rows] + both[rows:]


def received(blocks, slots, index_row, cell_count):
    width = blocks[0].shape[1]
    chooser = jnp.concatenate(
        [selector(index_row, cell_count + slot * width, width) for slot in slots], axis=0
    )
    return picked(jnp.concatenate([halves(block) for block in blocks], axis=1), chooser)


def steps(cell_count):
    width = STEP if cell_count % STEP == 0 else cell_count
    return [(at, at + width) for at in range(0, cell_count, width)]


def pack_kernel(flat_ref, send_ref, *out_refs):
    parts = halves(flat_ref[...])
    cell_count = parts.shape[1]
    for slot, out_ref in enumerate(by_slot(out_refs)):
        out_ref[...] = picked(parts, selector(send_ref[slot : slot + 1, :], 0, cell_count))


def near_kernel(flat_ref, near_ref, out_ref):
    parts = halves(flat_ref[...])
    cell_count = parts.shape[1]
    for edge in range(3):
        for lo, hi in steps(cell_count):
            chooser = selector(near_ref[edge : edge + 1, lo:hi], 0, cell_count)
            out_ref[edge, :, lo:hi] = picked(parts, chooser)


def gradient_kernel(peer_count, flat_ref, own_ref, lsq_ref, near_ref, send_ref, *refs):
    got_refs = refs[:peer_count]
    beside_ref, grad_ref = refs[peer_count : peer_count + 2]
    out_refs = refs[peer_count + 2 :]
    rows, cell_count = flat_ref.shape
    got = [ref[...] for ref in got_refs]
    slots = one_way(peer_count)
    for lo, hi in steps(cell_count):
        centre = flat_ref[:, lo:hi]
        sums = [None, None]
        for edge in range(3):
            index_row = near_ref[edge : edge + 1, lo:hi]
            value = own_ref[edge, :, lo:hi] + received(got, slots, index_row, cell_count)
            beside_ref[edge, :, lo:hi] = value
            change = value - centre
            for comp in range(2):
                term = lsq_ref[comp, edge : edge + 1, lo:hi] * change
                sums[comp] = term if sums[comp] is None else sums[comp] + term
        grad_ref[:rows, lo:hi] = sums[0]
        grad_ref[rows:, lo:hi] = sums[1]
    parts = halves(grad_ref[...])
    for slot, out_ref in enumerate(by_slot(out_refs)):
        out_ref[...] = picked(parts, selector(send_ref[slot : slot + 1, :], 0, cell_count))


def by_level(coeff, x):
    levels, width = coeff.shape
    return (x.reshape(x.shape[0] // levels, levels, width) * coeff[None]).reshape(x.shape)


def own_kernel(flat_ref, grad_ref, beside_ref, near_ref, flux_ref, own_off_ref, far_off_ref, far_ref, sum_ref):
    rows, cell_count = flat_ref.shape
    parts = halves(grad_ref[...])
    for lo, hi in steps(cell_count):
        centre = flat_ref[:, lo:hi]
        first = grad_ref[:rows, lo:hi]
        second = grad_ref[rows:, lo:hi]
        total = None
        for edge in range(3):
            chooser = selector(near_ref[edge : edge + 1, lo:hi], 0, cell_count)
            far = picked(parts, chooser)
            value = beside_ref[edge, :, lo:hi]
            far_ref[edge, :, lo:hi] = (
                value
                + by_level(far_off_ref[0, edge, :, lo:hi], far[:rows])
                + by_level(far_off_ref[1, edge, :, lo:hi], far[rows:])
            )
            face = (
                centre
                + by_level(own_off_ref[0, edge, :, lo:hi], first)
                + by_level(own_off_ref[1, edge, :, lo:hi], second)
            )
            face = jnp.clip(face, jnp.minimum(centre, value), jnp.maximum(centre, value))
            flow = by_level(jnp.maximum(flux_ref[edge, :, lo:hi], 0.0), face)
            total = flow if total is None else total + flow
        sum_ref[:, lo:hi] = total


def far_kernel(slots, flat_ref, beside_ref, far_ref, sum_ref, near_ref, flux_ref, far_off_ref, mass_ref, *refs):
    got_refs, out_ref = refs[:-1], refs[-1]
    rows, cell_count = flat_ref.shape
    got = [ref[...] for ref in got_refs]
    for lo, hi in steps(cell_count):
        centre = flat_ref[:, lo:hi]
        total = sum_ref[:, lo:hi]
        for edge in range(3):
            far = received(got, slots, near_ref[edge : edge + 1, lo:hi], cell_count)
            value = beside_ref[edge, :, lo:hi]
            face = (
                far_ref[edge, :, lo:hi]
                + by_level(far_off_ref[0, edge, :, lo:hi], far[:rows])
                + by_level(far_off_ref[1, edge, :, lo:hi], far[rows:])
            )
            face = jnp.clip(face, jnp.minimum(centre, value), jnp.maximum(centre, value))
            total = total + by_level(jnp.minimum(flux_ref[edge, :, lo:hi], 0.0), face)
        out_ref[:, lo:hi] = centre - by_level(mass_ref[:, lo:hi], total)


def first_kernel(slots, far_ref, near_ref, far_off_ref, *refs):
    got_refs, out_ref = refs[:-1], refs[-1]
    rows, cell_count = far_ref.shape[1:]
    got = [ref[...] for ref in got_refs]
    for lo, hi in steps(cell_count):
        for edge in range(3):
            far = received(got, slots, near_ref[edge : edge + 1, lo:hi], cell_count)
            out_ref[edge, :, lo:hi] = (
                far_ref[edge, :, lo:hi]
                + by_level(far_off_ref[0, edge, :, lo:hi], far[:rows])
                + by_level(far_off_ref[1, edge, :, lo:hi], far[rows:])
            )


def run(kernel, outs, flops, *operands):
    moved = sum(4 * x.size for x in operands) + sum(4 * x.size for x in outs)
    return pl.pallas_call(
        kernel,
        out_shape=outs,
        compiler_params=pltpu.CompilerParams(vmem_limit_bytes=GRANT),
        cost_estimate=pl.CostEstimate(flops=flops, bytes_accessed=moved, transcendentals=0),
    )(*operands)


def on_device(
    tracers, mass_flux, lsq_coeff, own_offset, far_offset, inv_mass, neighbour, send_cells
):
    tracer_count, level_count, cell_count = tracers.shape
    rows = tracer_count * level_count
    peer_count, halo_width = send_cells.shape
    halo_count = peer_count * halo_width
    flat = tracers.reshape(rows, cell_count)

    def like(*shape):
        return jax.ShapeDtypeStruct(shape, F32)

    def work(height, depth, width):
        return 4 * height * depth * width

    sent = run(
        pack_kernel,
        [like(rows, halo_width)] * peer_count,
        work(rows, cell_count, halo_count),
        flat,
        send_cells,
    )
    got = exchange(sent)
    own_beside = run(
        near_kernel,
        [like(3, rows, cell_count)],
        work(rows, cell_count, 3 * cell_count),
        flat,
        neighbour,
    )[0]
    beside, grad, *grad_sent = run(
        functools.partial(gradient_kernel, peer_count),
        [like(3, rows, cell_count), like(2 * rows, cell_count)]
        + [like(2 * rows, halo_width)] * peer_count,
        work(rows, halo_count, 5 * cell_count),
        flat,
        own_beside,
        lsq_coeff,
        neighbour,
        send_cells,
        *got,
    )
    grad_got = exchange(grad_sent)
    far_part, own_sum = run(
        own_kernel,
        [like(3, rows, cell_count), like(rows, cell_count)],
        work(2 * rows, cell_count, 3 * cell_count),
        flat,
        grad,
        beside,
        neighbour,
        mass_flux,
        own_offset,
        far_offset,
    )
    forward = (peer_count + 1) // 2
    slots = one_way(peer_count)
    far_part = run(
        functools.partial(first_kernel, slots[:forward]),
        [like(3, rows, cell_count)],
        work(rows, halo_count, 3 * cell_count),
        far_part,
        neighbour,
        far_offset,
        *grad_got[:forward],
    )[0]
    updated = run(
        functools.partial(far_kernel, slots[forward:]),
        [like(rows, cell_count)],
        work(2 * rows, halo_count, 3 * cell_count),
        flat,
        beside,
        far_part,
        own_sum,
        neighbour,
        mass_flux,
        far_offset,
        inv_mass,
        *grad_got[forward:],
    )[0]
    return updated.reshape(tracers.shape)


def solution(mesh):
    placed = (
        P(None, None, "dom"),
        P(None, None, "dom"),
        P(None, None, "dom"),
        P(None, None, None, "dom"),
        P(None, None, None, "dom"),
        P(None, "dom"),
        P(None, "dom"),
        P(None, "dom"),
    )
    return jax.shard_map(
        on_device, mesh=mesh, in_specs=placed, out_specs=P(None, None, "dom"), check_vma=False
    )
```
